32 devices in a mesh: gx: 8 (over z, y), gy: 4 (over x, core).
Axes of the slice: x: 2, y: 2, z: 4, core: 2. Of those that a mesh axis runs over, the one named last changes fastest.
Arguments:
- tokens: bfloat16 [256, 8192], P('gy', 'gx'), may hold values from -6 to 6
- target: bfloat16 [256, 8192], P('gy', 'gx'), may hold values from -6 to 6
- w_gate: bfloat16 [8192, 14336], P('gx', 'gy'), may hold values from -0.0625 to 0.0625
- w_up: bfloat16 [8192, 14336], P('gx', 'gy'), may hold values from -0.0625 to 0.0625
- w_down: bfloat16 [14336, 8192], P('gy', 'gx'), may hold values from -0.046875 to 0.046875
- t_gate: bfloat16 [8192, 14336], P('gx', 'gy'), may hold values from -0.0625 to 0.0625
- t_up: bfloat16 [8192, 14336], P('gx', 'gy'), may hold values from -0.0625 to 0.0625
- t_down: bfloat16 [14336, 8192], P('gy', 'gx'), may hold values from -0.046875 to 0.046875
Outputs:
- hvp_gate: bfloat16 [8192, 14336], P('gx', 'gy')
- hvp_up: bfloat16 [8192, 14336], P('gx', 'gy')
- hvp_down: bfloat16 [14336, 8192], P('gy', 'gx')
The draws below stay inside these ranges and needn't reach their ends.
All inputs are finite; a program needn't handle non-finite values.
Results may differ from the reference program's by a relative error of at most 0.0074.
Values may be sent and summed in bfloat16 or wider, within the bound.
A program may use at most 192 MiB of HBM per device.

```python
import math
import jax
import jax.numpy as jnp

D = 8192
FF = 14336
TOKENS = 256


def spiked(drawn, rng, source, target, blocks, factor):
    def block_of(position):
        return (jnp.arange(drawn.shape[position]) // (drawn.shape[position] // blocks)).reshape((-1,) + (1,) * (drawn.ndim - 1 - position))

    near = jax.random.permutation(rng, blocks)[block_of(target)]
    other_side = (block_of(target) + blocks // 2) % blocks
    return jnp.where((block_of(source) == near) | (block_of(source) == other_side), factor * drawn, drawn)


def levels(rng, extent, split, smallest, high):
    factor_of = 1.0
    for axis_at, parts in split:
        draws = jax.random.uniform(jax.random.fold_in(jax.random.fold_in(rng, 6), axis_at), (parts,), jnp.float32, smallest / len(split), high / len(split))
        factor_of = factor_of * jnp.repeat(jnp.exp(draws), extent[axis_at] // parts).reshape((-1,) + (1,) * (len(extent) - 1 - axis_at))
    return factor_of


def centred(own_key, extent, deviation, most, split=(), held_as=jnp.bfloat16):
    loudness = levels(own_key, extent, split, -0.22, 0.18) if split else 1.0
    result = jax.random.normal(own_key, extent, jnp.float32) * deviation * loudness
    return jnp.minimum(jnp.maximum(result, -most), most).astype(held_as)


def heavy_noise(stream_key, shape, spread, limit, shards, heavy, kind=jnp.bfloat16):
    array = spread * jax.random.normal(stream_key, shape, jnp.float32)
    if shards:
        array = array * levels(stream_key, shape, shards, -0.22, 0.18)
    return jnp.clip(spiked(array, jax.random.fold_in(stream_key, 3), *heavy), -limit, limit).astype(kind)


def setup_inputs(seed: int = 0) -> dict:
    key_of = jax.random.split(jax.random.key(seed), 9)
    tokens = heavy_noise(key_of[0], (TOKENS, D), 1.0, 6.0, ((0, 4), (1, 8)), (1, 0, 8, 2.0))
    target = centred(key_of[1], (TOKENS, D), 1.0, 6.0, ((0, 4), (1, 8)))
    w_gate = centred(key_of[2], (D, FF), D ** -0.5, 0.0625, ((0, 8), (1, 4)))
    w_up = centred(key_of[3], (D, FF), D ** -0.5, 0.0625, ((0, 8), (1, 4)))
    w_down = centred(key_of[4], (FF, D), FF ** -0.5, 0.046875, ((0, 4), (1, 8)))
    t_gate = centred(key_of[5], (D, FF), D ** -0.5, 0.0625, ((0, 8), (1, 4)))
    t_up = centred(key_of[6], (D, FF), D ** -0.5, 0.0625, ((0, 8), (1, 4)))
    t_down = centred(key_of[7], (FF, D), FF ** -0.5, 0.046875, ((0, 4), (1, 8)))
    return {"tokens": tokens, "target": target, "w_gate": w_gate, "w_up": w_up, "w_down": w_down, "t_gate": t_gate, "t_up": t_up, "t_down": t_down}


def silu_parts(gate):
    sig = jax.nn.sigmoid(gate)
    first = sig * (1.0 + gate * (1.0 - sig))
    second = sig * (1.0 - sig) * (2.0 + gate * (1.0 - 2.0 * sig))
    return (gate * sig, first, second)

def matmul(left, right):
    return jnp.dot(left, right, preferred_element_type=jnp.float32)

def reference(tokens, target, w_gate, w_up, w_down, t_gate, t_up, t_down):
    scale = 1.0 / math.sqrt(TOKENS)
    gate = matmul(tokens, w_gate)
    upper = matmul(tokens, w_up)
    gate_dot = matmul(tokens, t_gate)
    upper_dot = matmul(tokens, t_up)
    silu_val, first, second = silu_parts(gate)
    hidden = (silu_val * upper).astype(jnp.bfloat16)
    hidden_dot = (first * gate_dot * upper + silu_val * upper_dot).astype(jnp.bfloat16)
    output = matmul(hidden, w_down)
    output_dot = matmul(hidden_dot, w_down) + matmul(hidden, t_down)
    grad = ((output - target.astype(jnp.float32)) * scale).astype(jnp.bfloat16)
    grad_dot = (output_dot * scale).astype(jnp.bfloat16)
    hvp_down = (matmul(hidden_dot.T, grad) + matmul(hidden.T, grad_dot)).astype(jnp.bfloat16)
    back = matmul(grad, w_down.T)
    back_dot = matmul(grad_dot, w_down.T) + matmul(grad, t_down.T)
    gate_in = (back_dot * upper * first + back * upper_dot * first + back * upper * second * gate_dot).astype(jnp.bfloat16)
    upper_in = (back_dot * silu_val + back * first * gate_dot).astype(jnp.bfloat16)
    hvp_gate = matmul(tokens.T, gate_in).astype(jnp.bfloat16)
    hvp_up = matmul(tokens.T, upper_in).astype(jnp.bfloat16)
    return (hvp_gate, hvp_up, hvp_down)
```

```python
import functools
import math

import jax
import jax.numpy as jnp
from jax import lax
from jax.experimental import pallas as pl
from jax.experimental.pallas import tpu as pltpu
from jax.sharding import PartitionSpec as P

TOKENS = 256


def silu_parts(gate):
    sig = jax.nn.sigmoid(gate)
    first = sig * (1.0 + gate * (1.0 - sig))
    second = sig * (1.0 - sig) * (2.0 + gate * (1.0 - 2.0 * sig))
    return (gate * sig, first, second)


def matmul(left, right):
    return jnp.dot(left, right, preferred_element_type=jnp.float32)


def lead_dot(left, right):
    return lax.dot_general(
        left, right, (((0,), (0,)), ((), ())), preferred_element_type=jnp.float32
    )


def tail_dot(left, right):
    return lax.dot_general(
        left, right, (((1,), (1,)), ((), ())), preferred_element_type=jnp.float32
    )


def gather_kernel(axis, count, arrays, *refs):
    blocks, fulls = refs[:arrays], refs[arrays : 2 * arrays]
    own_sem, send, recv = refs[2 * arrays :]
    pairs = count // 2
    me = lax.axis_index(axis)
    side = lax.rem(me, 2)
    pair = lax.div(me, 2)
    partner = me + 1 - 2 * side
    peers = [lax.rem(pair + step, pairs) * 2 + side for step in range(1, pairs)]
    sources = [lax.rem(pair + pairs - step, pairs) * 2 + side for step in range(1, pairs)]
    rows = blocks[0].shape[0]

    def place(full, index):
        return full.at[pl.ds(pl.multiple_of(index * rows, rows), rows)]

    barrier = pltpu.get_barrier_semaphore()
    for peer in [partner, *peers]:
        pl.semaphore_signal(
            barrier, inc=1, device_id={axis: peer}, device_id_type=pl.DeviceIdType.MESH
        )
    pl.semaphore_wait(barrier, pairs)

    def remote(src, full, index, peer, slot):
        return pltpu.make_async_remote_copy(
            src_ref=src,
            dst_ref=place(full, index),
            send_sem=send.at[slot],
            recv_sem=recv.at[slot],
            device_id={axis: peer},
            device_id_type=pl.DeviceIdType.MESH,
        )

    slots = 2 * pairs - 1
    direct, final, own = {}, [], []
    for i in range(arrays):
        for step, peer in enumerate(peers):
            direct[i, step] = remote(blocks[i], fulls[i], me, peer, i * slots + step)
            direct[i, step].start()
        copy = remote(blocks[i], fulls[i], me, partner, i * slots + pairs - 1)
        copy.start()
        final.append(copy)
        own.append(pltpu.make_async_copy(blocks[i], place(fulls[i], me), own_sem.at[i]))
        own[-1].start()
    for i in range(arrays):
        for step, source in enumerate(sources):
            direct[i, step].wait_recv()
            copy = remote(
                place(fulls[i], source), fulls[i], source, partner, i * slots + pairs + step
            )
            copy.start()
            final.append(copy)
    for copy in direct.values():
        copy.wait_send()
    for copy in final + own:
        copy.wait()


def gather(blocks, axis, collective_id):
    count = lax.axis_size(axis)
    arrays = len(blocks)
    slots = arrays * (count - 1)
    sent = sum(block.size * 2 * (count - 1) for block in blocks)
    return pl.pallas_call(
        functools.partial(gather_kernel, axis, count, arrays),
        out_shape=[
            jax.ShapeDtypeStruct((count * block.shape[0], block.shape[1]), block.dtype)
            for block in blocks
        ],
        in_specs=[pl.BlockSpec(memory_space=pltpu.VMEM)] * arrays,
        out_specs=[pl.BlockSpec(memory_space=pl.ANY)] * arrays,
        scratch_shapes=[
            pltpu.SemaphoreType.DMA((arrays,)),
            pltpu.SemaphoreType.DMA((slots,)),
            pltpu.SemaphoreType.DMA((slots,)),
        ],
        compiler_params=pltpu.CompilerParams(
            collective_id=collective_id, has_side_effects=True
        ),
        cost_estimate=pl.CostEstimate(
            flops=0, bytes_accessed=16 * sent, transcendentals=0
        ),
    )(*blocks)


def products_kernel(turned, gate, upper, out_gate, out_up):
    out_gate[...] = matmul(turned[...], gate[...]).astype(out_gate.dtype)
    out_up[...] = matmul(turned[...], upper[...]).astype(out_up.dtype)


def weight_products(turned, gate, upper):
    rows, depth = turned.shape
    width = gate.shape[1]
    tile = next(size for size in (512, 256, 128) if width % size == 0)
    return pl.pallas_call(
        products_kernel,
        grid=(width // tile,),
        in_specs=[
            pl.BlockSpec((rows, depth), lambda i: (0, 0)),
            pl.BlockSpec((depth, tile), lambda i: (0, i)),
            pl.BlockSpec((depth, tile), lambda i: (0, i)),
        ],
        out_specs=[pl.BlockSpec((rows, tile), lambda i: (0, i))] * 2,
        out_shape=[jax.ShapeDtypeStruct((rows, width), jnp.bfloat16)] * 2,
        cost_estimate=pl.CostEstimate(
            flops=4 * rows * depth * width,
            bytes_accessed=4 * (rows + depth) * width,
            transcendentals=0,
        ),
    )(turned, gate, upper)


def scatter_kernel(axis, count, arrays, *refs):
    parts, outs = refs[:arrays], refs[arrays : 2 * arrays]
    landed, held, got, send1, recv1, send2, recv2 = refs[2 * arrays :]
    pairs = count // 2
    me = lax.axis_index(axis)
    side = lax.rem(me, 2)
    pair = lax.div(me, 2)
    partner = me + 1 - 2 * side
    targets = [lax.rem(pair + step, pairs) * 2 for step in range(1, pairs)]
    peers = [target + side for target in targets]

    barrier = pltpu.get_barrier_semaphore()
    for peer in [partner, *peers]:
        pl.semaphore_signal(
            barrier, inc=1, device_id={axis: peer}, device_id_type=pl.DeviceIdType.MESH
        )
    pl.semaphore_wait(barrier, pairs)

    first = {}
    for i in range(arrays):
        for k, target in enumerate([*targets, pair * 2]):
            first[i, k] = pltpu.make_async_remote_copy(
                src_ref=parts[i].at[target + 1 - side],
                dst_ref=landed.at[i, k],
                send_sem=send1.at[i * pairs + k],
                recv_sem=recv1.at[i * pairs + k],
                device_id={axis: partner},
                device_id_type=pl.DeviceIdType.MESH,
            )
            first[i, k].start()
    second = {}
    for i in range(arrays):
        for k, target in enumerate([*targets, pair * 2]):
            first[i, k].wait_recv()
            term = parts[i][target + side].astype(jnp.float32) + landed[i, k].astype(jnp.float32)
            if k == pairs - 1:
                outs[i][...] = term
                continue
            held[i, k] = term.astype(held.dtype)
            second[i, k] = pltpu.make_async_remote_copy(
                src_ref=held.at[i, k],
                dst_ref=got.at[i, k],
                send_sem=send2.at[i * pairs + k],
                recv_sem=recv2.at[i * pairs + k],
                device_id={axis: peers[k]},
                device_id_type=pl.DeviceIdType.MESH,
            )
            second[i, k].start()
    for i in range(arrays):
        for k in range(pairs - 1):
            second[i, k].wait_recv()
            outs[i][...] += got[i, k].astype(jnp.float32)
    for copy in [*first.values(), *second.values()]:
        copy.wait_send()


def scatter_sum(partials, axis, collective_id):
    count = lax.axis_size(axis)
    pairs = count // 2
    arrays = len(partials)
    rows, columns = partials[0].shape[0] // count, partials[0].shape[1]
    parts = [p.astype(jnp.bfloat16).reshape(count, rows, columns) for p in partials]
    sent = 2 * rows * columns * arrays * (count - 1)
    return pl.pallas_call(
        functools.partial(scatter_kernel, axis, count, arrays),
        out_shape=[jax.ShapeDtypeStruct((rows, columns), jnp.float32)] * arrays,
        in_specs=[pl.BlockSpec(memory_space=pltpu.VMEM)] * arrays,
        out_specs=[pl.BlockSpec(memory_space=pltpu.VMEM)] * arrays,
        scratch_shapes=[
            pltpu.VMEM((arrays, pairs, rows, columns), jnp.bfloat16),
            pltpu.VMEM((arrays, max(pairs - 1, 1), rows, columns), jnp.bfloat16),
            pltpu.VMEM((arrays, max(pairs - 1, 1), rows, columns), jnp.bfloat16),
            *[pltpu.SemaphoreType.DMA((arrays * pairs,))] * 4,
        ],
        compiler_params=pltpu.CompilerParams(
            collective_id=collective_id, has_side_effects=True
        ),
        cost_estimate=pl.CostEstimate(flops=0, bytes_accessed=16 * sent, transcendentals=0),
    )(*parts)


def body(tokens, target, w_gate, w_up, w_down, t_gate, t_up, t_down):
    scale = 1.0 / math.sqrt(TOKENS)
    (xfull,) = gather([tokens], "gy", 0)
    rows = xfull
    gate, upper, gate_dot, upper_dot = scatter_sum(
        [matmul(rows, w) for w in (w_gate, w_up, t_gate, t_up)], "gx", 4
    )
    silu_val, first, second = silu_parts(gate)
    hidden = (silu_val * upper).astype(jnp.bfloat16)
    hidden_dot = (first * gate_dot * upper + silu_val * upper_dot).astype(jnp.bfloat16)
    hid_full, hid_dot_full = gather([hidden, hidden_dot], "gx", 1)
    rows = hid_full
    rows_dot = hid_dot_full
    output = matmul(rows, w_down)
    output_dot = matmul(rows_dot, w_down) + matmul(rows, t_down)
    output, output_dot = scatter_sum([output, output_dot], "gy", 6)
    grad = ((output - target.astype(jnp.float32)) * scale).astype(jnp.bfloat16)
    grad_dot = (output_dot * scale).astype(jnp.bfloat16)
    grad_full, grad_dot_full = gather([grad, grad_dot], "gy", 2)
    hvp_down = (lead_dot(hid_dot_full, grad_full) + lead_dot(hid_full, grad_dot_full)).astype(
        jnp.bfloat16
    )
    rows = grad_full
    rows_dot = grad_dot_full
    back = tail_dot(rows, w_down)
    back_dot = tail_dot(rows_dot, w_down) + tail_dot(rows, t_down)
    back, back_dot = scatter_sum([back, back_dot], "gx", 5)
    gate_in = (
        back_dot * upper * first + back * upper_dot * first + back * upper * second * gate_dot
    ).astype(jnp.bfloat16)
    upper_in = (back_dot * silu_val + back * first * gate_dot).astype(jnp.bfloat16)
    gate_full, upper_full = gather([gate_in, upper_in], "gx", 3)
    hvp_gate, hvp_up = weight_products(lax.optimization_barrier(xfull.T), gate_full, upper_full)
    return (hvp_gate, hvp_up, hvp_down)


def solution(mesh):
    return jax.shard_map(
        body,
        mesh=mesh,
        in_specs=(
            P("gy", "gx"),
            P("gy", "gx"),
            P("gx", "gy"),
            P("gx", "gy"),
            P("gy", "gx"),
            P("gx", "gy"),
            P("gx", "gy"),
            P("gy", "gx"),
        ),
        out_specs=(P("gx", "gy"), P("gx", "gy"), P("gy", "gx")),
        check_vma=False,
    )
```
